128 devices in a mesh: dp: 8 (over x, core), tensor: 16 (over z, y).
Axes of the slice: x: 4, y: 4, z: 4, core: 2. Of those that a mesh axis runs over, the one named last changes fastest.
Arguments:
- activations: bfloat16 [4096, 28672], P('dp', 'tensor'), parts along dimension 0, may hold values from -6 to 6
- down_weight: bfloat16 [28672, 6144], P('tensor'), may hold values from -0.046875 to 0.046875
Outputs:
- projected: bfloat16 [4096, 6144], P(('dp', 'tensor')), parts along dimension 0
The draws below stay inside these ranges and needn't reach their ends.
There are 8 independent parts, one for each index of `dp`. The reference program is written for one: setup_inputs(seed, part) draws one part's arguments, and reference() takes and returns one part's arrays. A program takes and returns all parts, laid end to end along the dimension named above; an argument that names none is the same for every part. Nothing has to cross between parts.
All inputs are finite; a program needn't handle non-finite values.
Results may differ from the reference program's by a relative error of at most 0.015.
Values may be sent and summed in bfloat16 or wider, within the bound.
No kernel may reach another device: no remote copies, remote signals or barrier semaphores. Data moves between devices by JAX's collectives and lax.ppermute only.
A program may use at most 128 MiB of HBM per device.

```python
import math
import jax
import jax.numpy as jnp
import numpy as np
from jax import lax

SYL = 1024
FF = 28672
DW = 6144
TOK = 512


def with_spikes(result, stream_key, source, target, blocks, factor):
    def block_of(position):
        return (jnp.arange(result.shape[position]) // (result.shape[position] // blocks)).reshape((-1,) + (1,) * (result.ndim - 1 - position))

    near = jax.random.permutation(stream_key, blocks)[block_of(target)]
    far = (block_of(target) + blocks // 2) % blocks
    return jnp.where((block_of(source) == near) | (block_of(source) == far), factor * result, result)


def level_of(stream_key, extent, cuts, smallest, top_value):
    loudness, own = 1.0, jax.random.fold_in(stream_key, 6)
    for position, parts in cuts:
        draws = jnp.exp(jax.random.uniform(jax.random.fold_in(own, position), (parts,), jnp.float32, smallest / len(cuts), top_value / len(cuts)))
        loudness = loudness * jnp.repeat(draws, extent[position] // parts).reshape([-1 if axis == position else 1 for axis in range(len(extent))])
    return loudness


def normal_values(own_key, dims, scale, limit, cuts=(), held_as=jnp.bfloat16):
    gain = level_of(own_key, dims, cuts, -0.22, 0.18) if cuts else 1.0
    values = jax.random.normal(own_key, dims, jnp.float32) * scale * gain
    return jnp.minimum(jnp.maximum(values, -limit), limit).astype(held_as)


def noise_with(own_key, extent, scale, reach, shards, heavy, dtype=jnp.bfloat16):
    result = scale * jax.random.normal(own_key, extent, jnp.float32)
    if shards:
        result = result * level_of(own_key, extent, shards, -0.22, 0.18)
    return jnp.clip(with_spikes(result, jax.random.fold_in(own_key, 3), *heavy), -reach, reach).astype(dtype)


def setup_inputs(seed: int = 0, part: int = 0) -> dict:
    arg_keys = jax.random.split(jax.random.key(seed), 3)
    own_keys = jax.random.split(jax.random.fold_in(arg_keys[2], part), 3)
    return {
        "activations": normal_values(own_keys[0], (TOK, FF), 1.0, 6.0, ((1, 16),)),
        "down_weight": noise_with(arg_keys[1], (FF, DW), FF ** -0.5, 0.046875, ((0, 16),), (0, 1, 16, 2.0)),
    }


def paley_matrix():
    modulus = 13
    residues = set((value * value % modulus for value in range(1, modulus)))
    jacobsthal = np.array([[0.0 if row_at == col_at else 1.0 if (col_at - row_at) % modulus in residues else -1.0 for col_at in range(modulus)] for row_at in range(modulus)])
    confer = np.zeros((14, 14))
    confer[0, 1:] = 1.0
    confer[1:, 0] = 1.0
    confer[1:, 1:] = jacobsthal
    return np.kron(confer, np.array([[1.0, 1.0], [1.0, -1.0]])) + np.kron(np.eye(14), np.array([[1.0, -1.0], [-1.0, -1.0]]))

def sylvester(order):
    matrix = np.ones((1, 1))
    while matrix.shape[0] < order:
        matrix = np.kron(matrix, np.array([[1.0, 1.0], [1.0, -1.0]]))
    return matrix

def quantize(rotated, largest):
    token_scale = jnp.maximum(largest, 1.0)
    levels = 7.0 * rotated / token_scale
    snapped = levels - jnp.sin(2.0 * math.pi * levels) / (2.0 * math.pi)
    return (snapped * token_scale / 7.0).astype(jnp.bfloat16)

def reference(activations, down_weight):
    count_rows = activations.shape[0]
    small_table = jnp.asarray(paley_matrix(), jnp.float32)
    power_table = jnp.asarray(sylvester(SYL), jnp.float32)
    values = activations.astype(jnp.float32).reshape(count_rows * SYL, 28)
    inner = jnp.dot(values, small_table, precision=lax.Precision.HIGHEST).reshape(count_rows, SYL, 28)
    outer = jnp.einsum('tji,jk->tki', inner, power_table, precision=lax.Precision.HIGHEST)
    rotated = outer.reshape(count_rows, FF) * (1.0 / math.sqrt(FF))
    largest = lax.optimization_barrier(jnp.max(jnp.abs(rotated), axis=1, keepdims=True))
    dequant = quantize(rotated, largest)
    return jnp.dot(dequant, down_weight, preferred_element_type=jnp.float32).astype(jnp.bfloat16)
```

```python
import functools
import math

import jax
import jax.numpy as jnp
import numpy as np
from jax import lax
from jax.experimental import pallas as pl
from jax.experimental.pallas import tpu as pltpu
from jax.sharding import PartitionSpec as P


def paley_matrix():
    modulus = 13
    residues = set((value * value % modulus for value in range(1, modulus)))
    jacobsthal = np.array(
        [
            [
                (
                    0.0
                    if row_at == col_at
                    else 1.0 if (col_at - row_at) % modulus in residues else -1.0
                )
                for col_at in range(modulus)
            ]
            for row_at in range(modulus)
        ]
    )
    confer = np.zeros((14, 14))
    confer[0, 1:] = 1.0
    confer[1:, 0] = 1.0
    confer[1:, 1:] = jacobsthal
    return np.kron(confer, np.array([[1.0, 1.0], [1.0, -1.0]])) + np.kron(
        np.eye(14), np.array([[1.0, -1.0], [-1.0, -1.0]])
    )


def sylvester(order):
    matrix = np.ones((1, 1))
    while matrix.shape[0] < order:
        matrix = np.kron(matrix, np.array([[1.0, 1.0], [1.0, -1.0]]))
    return matrix


HALF = 896


def rotate_kernel(act_ref, table_ref, out_ref):
    table = table_ref[...]
    low = jnp.dot(act_ref[:, :HALF], table, preferred_element_type=jnp.float32)
    high = jnp.dot(act_ref[:, HALF:], table, preferred_element_type=jnp.float32)
    out_ref[:, :HALF] = (low + high).astype(jnp.bfloat16)
    out_ref[:, HALF:] = (low - high).astype(jnp.bfloat16)


def rotate(activations):
    rows, width = activations.shape
    table = jnp.asarray(np.kron(sylvester(32), paley_matrix()), jnp.bfloat16)
    step = 128
    return pl.pallas_call(
        rotate_kernel,
        grid=(rows // step,),
        in_specs=[
            pl.BlockSpec((step, width), lambda i: (i, 0)),
            pl.BlockSpec((HALF, HALF), lambda i: (0, 0)),
        ],
        out_specs=pl.BlockSpec((step, width), lambda i: (i, 0)),
        out_shape=jax.ShapeDtypeStruct((rows, width), jnp.bfloat16),
        name="rotate",
    )(activations, table)


def sine_coefs():
    nodes = np.cos(np.pi * (np.arange(400) + 0.5) / 400) * 0.125 + 0.125
    x = np.sqrt(nodes)
    values = np.sin(2 * np.pi * x) / (2 * np.pi * x)
    return np.polynomial.chebyshev.Chebyshev.fit(
        nodes, values, 7, domain=[0, 0.25]
    ).convert(kind=np.polynomial.Polynomial).coef


COEFS = [float(c) for c in sine_coefs()]


def snap(levels):
    rest = levels - jnp.round(levels)
    square = rest * rest
    poly = jnp.full_like(square, COEFS[-1])
    for coef in COEFS[-2::-1]:
        poly = poly * square + coef
    return levels - rest * poly


def quantize_kernel(mixed_ref, out_ref, rot_ref, *, norm):
    groups, rows, width = mixed_ref.shape
    lanes = 128
    sub = 16
    for row in range(0, rows, sub):
        def mix(c, top, row=row):
            at = pl.ds(pl.multiple_of(c * lanes, lanes), lanes)
            v = [mixed_ref[e, row : row + sub, at].astype(jnp.float32) for e in range(groups)]
            stride = 1
            while stride < groups:
                for e in range(groups):
                    if not e & stride:
                        v[e], v[e + stride] = v[e] + v[e + stride], v[e] - v[e + stride]
                stride *= 2
            for e in range(groups):
                rot_ref[e, row : row + sub, at] = v[e]
                top = jnp.maximum(top, jnp.abs(v[e]))
            return top

        top = lax.fori_loop(0, width // lanes, mix, jnp.zeros((sub, lanes), jnp.float32))
        scale = jnp.maximum(jnp.max(top, axis=1, keepdims=True) * norm, 1.0)
        into = jnp.broadcast_to((7.0 * norm) / scale, (sub, lanes))
        back = jnp.broadcast_to(scale / 7.0, (sub, lanes))

        def quant(c, carry, row=row, into=into, back=back):
            at = pl.ds(pl.multiple_of(c * lanes, lanes), lanes)
            for e in range(groups):
                levels = rot_ref[e, row : row + sub, at] * into
                out_ref[e, row : row + sub, at] = (snap(levels) * back).astype(jnp.bfloat16)
            return carry

        lax.fori_loop(0, width // lanes, quant, 0)


def quantize(mixed, norm):
    return pl.pallas_call(
        functools.partial(quantize_kernel, norm=norm),
        in_specs=[pl.BlockSpec(memory_space=pltpu.VMEM)],
        out_specs=pl.BlockSpec(memory_space=pltpu.VMEM),
        out_shape=jax.ShapeDtypeStruct(mixed.shape, jnp.bfloat16),
        scratch_shapes=[pltpu.VMEM(mixed.shape, jnp.float32)],
        name="quantize",
    )(mixed)


SIDE = 4


def shift(value, along, by):
    pairs = []
    for z in range(SIDE):
        for y in range(SIDE):
            to = ((z + by) % SIDE, y) if along == "z" else (z, (y + by) % SIDE)
            pairs.append((SIDE * z + y, SIDE * to[0] + to[1]))
    return lax.ppermute(value, "tensor", pairs)


TILE = 768


def project_kernel(place_ref, values_ref, weight_ref, up_ref, down_ref, mid_ref, own_ref, lhs_ref, *, along):
    step = pl.program_id(0)
    z, y = place_ref[0], place_ref[1]
    rows = values_ref.shape[0] // (SIDE * SIDE)
    group = SIDE * rows

    @pl.when(step == 0)
    def _():
        for r in range(SIDE):
            if along == "z":
                start = pl.multiple_of(((z + r) % SIDE) * group, group)
                lhs_ref[r * group : (r + 1) * group, :] = values_ref[pl.ds(start, group), :]
            else:
                for other in range(SIDE):
                    start = pl.multiple_of(other * group + ((y + r) % SIDE) * rows, rows)
                    to = r * group + other * rows
                    lhs_ref[to : to + rows, :] = values_ref[pl.ds(start, rows), :]

    def part(r, count=1):
        lhs = lhs_ref[r * group : (r + count) * group, :]
        return jnp.dot(lhs, weight_ref[...], preferred_element_type=jnp.float32).astype(jnp.bfloat16)

    whole = part(0, SIDE)
    own_ref[...] = whole[:group]
    ahead, far, behind = whole[group : 2 * group], whole[2 * group : 3 * group], whole[3 * group :]
    low = step < pl.num_programs(0) // 2

    @pl.when(low)
    def _():
        up_ref[...] = far
        down_ref[...] = behind
        mid_ref[...] = ahead

    @pl.when(jnp.logical_not(low))
    def _():
        up_ref[...] = ahead
        down_ref[...] = far
        mid_ref[...] = behind


def project(values, weight, place, along, first):
    count_rows, width = values.shape
    columns = weight.shape[1] // 2
    group = count_rows // SIDE
    offset = first // TILE
    out = jax.ShapeDtypeStruct((group, columns), jnp.bfloat16)
    block = pl.BlockSpec((group, TILE), lambda j, place: (0, j))
    return pl.pallas_call(
        functools.partial(project_kernel, along=along),
        grid_spec=pltpu.PrefetchScalarGridSpec(
            num_scalar_prefetch=1,
            grid=(columns // TILE,),
            in_specs=[
                pl.BlockSpec((count_rows, width), lambda j, place: (0, 0)),
                pl.BlockSpec((width, TILE), lambda j, place: (0, j + offset)),
            ],
            out_specs=[block] * 4,
            scratch_shapes=[pltpu.VMEM((count_rows, width), jnp.bfloat16)],
        ),
        out_shape=[out] * 4,
        name="project_" + along,
    )(place, values, weight)


def f32(value):
    return value.astype(jnp.float32)


def split_kernel(place_ref, own_ref, up_ref, down_ref, up2_ref, down2_ref, *outs, index):
    up_out, down_out, mid_out, own_out = outs
    at = place_ref[index]
    rows, half = own_out.shape[0], own_out.shape[1] // 2
    low, high = slice(0, half), slice(half, 2 * half)
    targets = ((own_out, own_out), (mid_out, up_out), (up_out, down_out), (down_out, mid_out))
    for r in range(SIDE):
        take = pl.ds(pl.multiple_of(((at + r) % SIDE) * rows, rows), rows)
        targets[r][0][:, low] = (
            f32(own_ref[take, low]) + f32(down_ref[take, low]) + f32(up2_ref[take, :])
        ).astype(jnp.bfloat16)
        targets[r][1][:, high] = (
            f32(own_ref[take, high]) + f32(up_ref[take, high]) + f32(down2_ref[take, :])
        ).astype(jnp.bfloat16)


def split(place, index, own, up, down, up2, down2):
    vmem = pl.BlockSpec(memory_space=pltpu.VMEM)
    out = jax.ShapeDtypeStruct((own.shape[0] // SIDE, own.shape[1]), jnp.bfloat16)
    return pl.pallas_call(
        functools.partial(split_kernel, index=index),
        in_specs=[pl.BlockSpec(memory_space=pltpu.SMEM)] + [vmem] * 5,
        out_specs=[vmem] * 4,
        out_shape=[out] * 4,
        name="split",
    )(place, own, up, down, up2, down2)


def relay_kernel(mid_ref, up_ref, down_ref, up2_ref, down2_ref):
    half = up2_ref.shape[1]
    up2_ref[...] = (f32(mid_ref[:, :half]) + f32(up_ref[:, :half])).astype(jnp.bfloat16)
    down2_ref[...] = (f32(mid_ref[:, half:]) + f32(down_ref[:, half:])).astype(jnp.bfloat16)


def relay(mid, up, down):
    vmem = pl.BlockSpec(memory_space=pltpu.VMEM)
    out = jax.ShapeDtypeStruct((mid.shape[0], mid.shape[1] // 2), jnp.bfloat16)
    return pl.pallas_call(
        relay_kernel, in_specs=[vmem] * 3, out_specs=[vmem] * 2, out_shape=[out] * 2, name="relay"
    )(mid, up, down)


def finish_kernel(*refs):
    out_ref = refs[-1]
    half = refs[3].shape[1]
    for at in range(2):
        own, up, down, up2, down2 = refs[5 * at : 5 * at + 5]
        base = 2 * half * at
        out_ref[:, base : base + half] = (
            f32(own[:, :half]) + f32(down[:, :half]) + f32(up2[...])
        ).astype(jnp.bfloat16)
        out_ref[:, base + half : base + 2 * half] = (
            f32(own[:, half:]) + f32(up[:, half:]) + f32(down2[...])
        ).astype(jnp.bfloat16)


def finish(first, second):
    vmem = pl.BlockSpec(memory_space=pltpu.VMEM)
    own = first[0]
    out = jax.ShapeDtypeStruct((own.shape[0], 2 * own.shape[1]), jnp.bfloat16)
    return pl.pallas_call(
        finish_kernel, in_specs=[vmem] * 10, out_specs=vmem, out_shape=out, name="finish"
    )(*first, *second)


def ring(up, down, mid, own, along):
    got_up = shift(up, along, 1)
    got_down = shift(down, along, -1)
    up2, down2 = relay(mid, got_up, got_down)
    return own, got_up, got_down, shift(up2, along, 1), shift(down2, along, -1)


def shards(activations, down_weight):
    count_rows, shard_width = activations.shape
    groups = lax.axis_size("tensor")
    me = lax.axis_index("tensor")
    place = jnp.stack([me // SIDE, me % SIDE]).astype(jnp.int32)
    blocks = rotate(activations).reshape(groups, count_rows // groups, shard_width)
    mixed = lax.all_to_all(blocks, "tensor", split_axis=0, concat_axis=0, tiled=True)
    snapped = quantize(mixed, 1.0 / math.sqrt(shard_width * groups))
    values = lax.all_to_all(snapped, "tensor", split_axis=0, concat_axis=0, tiled=True)
    values = values.reshape(count_rows, shard_width)
    half = down_weight.shape[1] // 2
    first_z = ring(*project(values, down_weight, place, "z", 0), "z")
    first_y = ring(*project(values, down_weight, place, "y", half), "y")
    second_y = ring(*split(place, 1, *first_z), "y")
    second_z = ring(*split(place, 0, *first_y), "z")
    return finish(second_y, second_z)


def solution(mesh):
    placed = (P("dp", "tensor"), P("tensor", None))
    return jax.shard_map(
        shards, mesh=mesh, in_specs=placed, out_specs=P(("dp", "tensor"), None), check_vma=False
    )
```

```python
import functools
import math

import jax
import jax.numpy as jnp
import numpy as np
from jax import lax
from jax.experimental import pallas as pl
from jax.experimental.pallas import tpu as pltpu
from jax.sharding import PartitionSpec as P


def paley_matrix():
    modulus = 13
    residues = set((value * value % modulus for value in range(1, modulus)))
    jacobsthal = np.array(
        [
            [
                (
                    0.0
                    if row_at == col_at
                    else 1.0 if (col_at - row_at) % modulus in residues else -1.0
                )
                for col_at in range(modulus)
            ]
            for row_at in range(modulus)
        ]
    )
    confer = np.zeros((14, 14))
    confer[0, 1:] = 1.0
    confer[1:, 0] = 1.0
    confer[1:, 1:] = jacobsthal
    return np.kron(confer, np.array([[1.0, 1.0], [1.0, -1.0]])) + np.kron(
        np.eye(14), np.array([[1.0, -1.0], [-1.0, -1.0]])
    )


def sylvester(order):
    matrix = np.ones((1, 1))
    while matrix.shape[0] < order:
        matrix = np.kron(matrix, np.array([[1.0, 1.0], [1.0, -1.0]]))
    return matrix


def small(mebibytes=6):
    return pltpu.CompilerParams(vmem_limit_bytes=mebibytes << 20)


HALF = 896


STEPS = 4
PIECES = 4


def weight_copies(weight_ref, out_ref, sems, first):
    rows = weight_ref.shape[0] // PIECES
    return [
        pltpu.make_async_copy(
            weight_ref.at[pl.ds(i * rows, rows), pl.ds(first, out_ref.shape[1])],
            out_ref.at[pl.ds(i * rows, rows)],
            sems.at[i],
        )
        for i in range(PIECES)
    ]


def rotate_kernel(act_hbm, table_hbm, weight_hbm, out_ref, weight_ref, act_ref, table_ref, sems, weight_sems):
    rows = act_hbm.shape[0] // STEPS
    bring_table = pltpu.make_async_copy(table_hbm, table_ref, sems.at[STEPS])
    bring = [
        pltpu.make_async_copy(
            act_hbm.at[pl.ds(i * rows, rows)], act_ref.at[pl.ds(i * rows, rows)], sems.at[i]
        )
        for i in range(STEPS)
    ]
    bring_weight = weight_copies(weight_hbm, weight_ref, weight_sems, 0)
    bring_table.start()
    for copy in bring + bring_weight:
        copy.start()
    bring_table.wait()
    for i, copy in enumerate(bring):
        copy.wait()
        at = slice(i * rows, (i + 1) * rows)
        low = jnp.dot(act_ref[at, :HALF], table_ref[...], preferred_element_type=jnp.float32)
        high = jnp.dot(act_ref[at, HALF:], table_ref[...], preferred_element_type=jnp.float32)
        out_ref[at, :HALF] = (low + high).astype(jnp.bfloat16)
        out_ref[at, HALF:] = (low - high).astype(jnp.bfloat16)
    for copy in bring_weight:
        copy.wait()


def rotate(activations, weight):
    table = jnp.asarray(np.kron(sylvester(32), paley_matrix()), jnp.bfloat16)
    hbm = pl.BlockSpec(memory_space=pltpu.HBM)
    vmem = pl.BlockSpec(memory_space=pltpu.VMEM)
    half = jax.ShapeDtypeStruct((weight.shape[0], weight.shape[1] // 2), weight.dtype)
    return pl.pallas_call(
        rotate_kernel,
        in_specs=[hbm] * 3,
        out_specs=[vmem] * 2,
        out_shape=[jax.ShapeDtypeStruct(activations.shape, jnp.bfloat16), half],
        scratch_shapes=[
            pltpu.VMEM(activations.shape, jnp.bfloat16),
            pltpu.VMEM(table.shape, jnp.bfloat16),
            pltpu.SemaphoreType.DMA((STEPS + 1,)),
            pltpu.SemaphoreType.DMA((PIECES,)),
        ],
        name="rotate",
        compiler_params=small(8),
    )(*[pltpu.with_memory_space_constraint(value, pltpu.HBM) for value in (activations, table, weight)])


def sine_coefs():
    nodes = np.cos(np.pi * (np.arange(400) + 0.5) / 400) * 0.125 + 0.125
    x = np.sqrt(nodes)
    values = np.sin(2 * np.pi * x) / (2 * np.pi * x)
    return np.polynomial.chebyshev.Chebyshev.fit(
        nodes, values, 7, domain=[0, 0.25]
    ).convert(kind=np.polynomial.Polynomial).coef


COEFS = [float(c) for c in sine_coefs()]


def snap(levels):
    rest = levels - jnp.round(levels)
    square = rest * rest
    poly = jnp.full_like(square, COEFS[-1])
    for coef in COEFS[-2::-1]:
        poly = poly * square + coef
    return levels - rest * poly


def quantize_kernel(mixed_ref, weight_hbm, out_ref, weight_ref, rot_ref, weight_sems, *, norm):
    bring_weight = weight_copies(weight_hbm, weight_ref, weight_sems, weight_ref.shape[1])
    for copy in bring_weight:
        copy.start()
    groups, rows, width = mixed_ref.shape
    lanes = 128
    sub = 16
    for row in range(0, rows, sub):
        def mix(c, top, row=row):
            at = pl.ds(pl.multiple_of(c * lanes, lanes), lanes)
            v = [mixed_ref[e, row : row + sub, at].astype(jnp.float32) for e in range(groups)]
            stride = 1
            while stride < groups:
                for e in range(groups):
                    if not e & stride:
                        v[e], v[e + stride] = v[e] + v[e + stride], v[e] - v[e + stride]
                stride *= 2
            for e in range(groups):
                rot_ref[e, row : row + sub, at] = v[e]
                top = jnp.maximum(top, jnp.abs(v[e]))
            return top

        top = lax.fori_loop(0, width // lanes, mix, jnp.zeros((sub, lanes), jnp.float32))
        scale = jnp.maximum(jnp.max(top, axis=1, keepdims=True) * norm, 1.0)
        into = jnp.broadcast_to((7.0 * norm) / scale, (sub, lanes))
        back = jnp.broadcast_to(scale / 7.0, (sub, lanes))

        def quant(c, carry, row=row, into=into, back=back):
            at = pl.ds(pl.multiple_of(c * lanes, lanes), lanes)
            for e in range(groups):
                levels = rot_ref[e, row : row + sub, at] * into
                out_ref[e, row : row + sub, at] = (snap(levels) * back).astype(jnp.bfloat16)
            return carry

        lax.fori_loop(0, width // lanes, quant, 0)
    for copy in bring_weight:
        copy.wait()


def quantize(mixed, weight, norm):
    vmem = pl.BlockSpec(memory_space=pltpu.VMEM)
    half = jax.ShapeDtypeStruct((weight.shape[0], weight.shape[1] // 2), weight.dtype)
    return pl.pallas_call(
        functools.partial(quantize_kernel, norm=norm),
        in_specs=[vmem, pl.BlockSpec(memory_space=pltpu.HBM)],
        out_specs=[vmem] * 2,
        out_shape=[jax.ShapeDtypeStruct(mixed.shape, jnp.bfloat16), half],
        scratch_shapes=[pltpu.VMEM(mixed.shape, jnp.float32), pltpu.SemaphoreType.DMA((PIECES,))],
        name="quantize",
        compiler_params=small(8),
    )(mixed, pltpu.with_memory_space_constraint(weight, pltpu.HBM))


SIDE = 4


def shift(value, along, by):
    pairs = []
    for z in range(SIDE):
        for y in range(SIDE):
            to = ((z + by) % SIDE, y) if along == "z" else (z, (y + by) % SIDE)
            pairs.append((SIDE * z + y, SIDE * to[0] + to[1]))
    return lax.ppermute(value, "tensor", pairs)


def project_kernel(place_ref, values_ref, weight_ref, first_ref, second_ref, lhs_ref, *, along, send):
    z, y = place_ref[0], place_ref[1]
    rows = values_ref.shape[0] // (SIDE * SIDE)
    group = SIDE * rows
    base = 1 if send else 3
    for r in range(3):
        if along == "z":
            start = pl.multiple_of(((z + base + r) % SIDE) * group, group)
            lhs_ref[r * group : (r + 1) * group, :] = values_ref[pl.ds(start, group), :]
        else:
            for other in range(SIDE):
                start = pl.multiple_of(other * group + ((y + base + r) % SIDE) * rows, rows)
                to = r * group + other * rows
                lhs_ref[to : to + rows, :] = values_ref[pl.ds(start, rows), :]
    half = weight_ref.shape[1] // 2
    for at in range(0, 2 * half, TILE):
        start = group if at < half else 0
        both = jnp.dot(
            lhs_ref[start : start + 2 * group, :],
            weight_ref[:, at : at + TILE],
            preferred_element_type=jnp.float32,
        ).astype(jnp.bfloat16)
        first_ref[:, at : at + TILE] = both[:group]
        second_ref[:, at : at + TILE] = both[group:]


TILE = 512


def project(values, weight, place, along, send):
    count_rows, width = values.shape
    group = count_rows // SIDE
    out = jax.ShapeDtypeStruct((group, weight.shape[1]), jnp.bfloat16)
    vmem = pl.BlockSpec(memory_space=pltpu.VMEM)
    return pl.pallas_call(
        functools.partial(project_kernel, along=along, send=send),
        in_specs=[pl.BlockSpec(memory_space=pltpu.SMEM), vmem, vmem],
        out_specs=[vmem] * 2,
        out_shape=[out] * 2,
        scratch_shapes=[pltpu.VMEM((3 * group, width), jnp.bfloat16)],
        name=("send_" if send else "keep_") + along,
        compiler_params=small(8),
    )(place, values, weight)


def f32(value):
    return value.astype(jnp.float32)


def split_kernel(place_ref, first_ref, second_ref, up_ref, down_ref, up2_ref, down2_ref, *outs, index):
    at = place_ref[index]
    rows, half = outs[0].shape[0], outs[0].shape[1] // 2
    low, high = slice(0, half), slice(half, 2 * half)
    for r in range(SIDE):
        take = pl.ds(pl.multiple_of(((at + r) % SIDE) * rows, rows), rows)
        outs[r][:, low] = (
            f32(first_ref[take, low]) + f32(down_ref[take, low]) + f32(up2_ref[take, :])
        ).astype(jnp.bfloat16)
        outs[r][:, high] = (
            f32(second_ref[take, high]) + f32(up_ref[take, high]) + f32(down2_ref[take, :])
        ).astype(jnp.bfloat16)


def split(place, index, first, second, up, down, up2, down2):
    vmem = pl.BlockSpec(memory_space=pltpu.VMEM)
    out = jax.ShapeDtypeStruct((first.shape[0] // SIDE, first.shape[1]), jnp.bfloat16)
    return pl.pallas_call(
        functools.partial(split_kernel, index=index),
        in_specs=[pl.BlockSpec(memory_space=pltpu.SMEM)] + [vmem] * 6,
        out_specs=[vmem] * 4,
        out_shape=[out] * 4,
        name="split",
        compiler_params=small(),
    )(place, first, second, up, down, up2, down2)


def relay_kernel(first_ref, second_ref, up_ref, down_ref, up2_ref, down2_ref):
    half = up2_ref.shape[1]
    up2_ref[...] = (f32(second_ref[:, :half]) + f32(up_ref[:, :half])).astype(jnp.bfloat16)
    down2_ref[...] = (f32(first_ref[:, half:]) + f32(down_ref[:, half:])).astype(jnp.bfloat16)


def relay(first, second, up, down):
    vmem = pl.BlockSpec(memory_space=pltpu.VMEM)
    out = jax.ShapeDtypeStruct((first.shape[0], first.shape[1] // 2), jnp.bfloat16)
    return pl.pallas_call(
        relay_kernel, in_specs=[vmem] * 4, out_specs=[vmem] * 2, out_shape=[out] * 2, name="relay",
        compiler_params=small(),
    )(first, second, up, down)


def finish_kernel(*refs):
    out_ref = refs[-1]
    width = refs[0].shape[1]
    for at in range(2):
        parts = [f32(ref[...]) for ref in refs[SIDE * at : SIDE * at + SIDE]]
        out_ref[:, width * at : width * at + width] = (
            (parts[0] + parts[1]) + (parts[2] + parts[3])
        ).astype(jnp.bfloat16)


def finish(first, second):
    vmem = pl.BlockSpec(memory_space=pltpu.VMEM)
    own = first[0]
    out = jax.ShapeDtypeStruct((own.shape[0], 2 * own.shape[1]), jnp.bfloat16)
    return pl.pallas_call(
        finish_kernel, in_specs=[vmem] * 8, out_specs=vmem, out_shape=out, name="finish",
        compiler_params=small(),
    )(*first, *second)


def exchange(own, ahead, far, behind, along):
    return own, shift(far, along, 2), shift(ahead, along, 1), shift(behind, along, -1)


def shards(activations, down_weight):
    count_rows, shard_width = activations.shape
    groups = lax.axis_size("tensor")
    me = lax.axis_index("tensor")
    place = jnp.stack([me // SIDE, me % SIDE]).astype(jnp.int32)
    activations, place = lax.optimization_barrier((activations, place))
    blocks, weight_z = rotate(activations, down_weight)
    blocks = blocks.reshape(groups, count_rows // groups, shard_width)
    mixed = lax.all_to_all(blocks, "tensor", split_axis=0, concat_axis=0, tiled=True)
    snapped, weight_y = quantize(mixed, down_weight, 1.0 / math.sqrt(shard_width * groups))
    values = lax.all_to_all(snapped, "tensor", split_axis=0, concat_axis=0, tiled=True)
    values = values.reshape(count_rows, shard_width)
    order = (("y", weight_y), ("z", weight_z))
    sent, kept = {}, {}
    for along, weight in order:
        up, down = project(values, weight, place, along, True)
        sent[along] = shift(up, along, 1), shift(down, along, -1)
    for along, weight in order:
        kept[along] = project(values, weight, place, along, False)
    ends = {}
    for along, _ in order:
        up, down = sent[along]
        up2, down2 = relay(*kept[along], up, down)
        ends[along] = (*kept[along], up, down, shift(up2, along, 1), shift(down2, along, -1))
    second_z = exchange(*split(place, 0, *ends["y"]), "z")
    second_y = exchange(*split(place, 1, *ends["z"]), "y")
    return finish(second_y, second_z)


def solution(mesh):
    placed = (P("dp", "tensor"), P("tensor", None))
    return jax.shard_map(
        shards, mesh=mesh, in_specs=placed, out_specs=P(("dp", "tensor"), None), check_vma=False
    )
```

```python
import functools
import math

import jax
import jax.numpy as jnp
import numpy as np
from jax import lax
from jax.experimental import pallas as pl
from jax.experimental.pallas import tpu as pltpu
from jax.sharding import PartitionSpec as P


def paley_matrix():
    modulus = 13
    residues = set((value * value % modulus for value in range(1, modulus)))
    jacobsthal = np.array(
        [
            [
                (
                    0.0
                    if row_at == col_at
                    else 1.0 if (col_at - row_at) % modulus in residues else -1.0
                )
                for col_at in range(modulus)
            ]
            for row_at in range(modulus)
        ]
    )
    confer = np.zeros((14, 14))
    confer[0, 1:] = 1.0
    confer[1:, 0] = 1.0
    confer[1:, 1:] = jacobsthal
    return np.kron(confer, np.array([[1.0, 1.0], [1.0, -1.0]])) + np.kron(
        np.eye(14), np.array([[1.0, -1.0], [-1.0, -1.0]])
    )


def sylvester(order):
    matrix = np.ones((1, 1))
    while matrix.shape[0] < order:
        matrix = np.kron(matrix, np.array([[1.0, 1.0], [1.0, -1.0]]))
    return matrix


def small(mebibytes=6):
    return pltpu.CompilerParams(vmem_limit_bytes=mebibytes << 20)


HALF = 896


STEPS = 4
LATER = 2816
PIECES = 4


def weight_copies(weight_ref, out_ref, sems, first):
    rows = weight_ref.shape[0] // PIECES
    return [
        pltpu.make_async_copy(
            weight_ref.at[pl.ds(i * rows, rows), pl.ds(first, out_ref.shape[1])],
            out_ref.at[pl.ds(i * rows, rows)],
            sems.at[i],
        )
        for i in range(PIECES)
    ]


def rotate_kernel(act_hbm, table_hbm, weight_hbm, out_ref, weight_ref, act_ref, table_ref, sems, weight_sems):
    rows = act_hbm.shape[0] // STEPS
    bring_table = pltpu.make_async_copy(table_hbm, table_ref, sems.at[STEPS])
    bring = [
        pltpu.make_async_copy(
            act_hbm.at[pl.ds(i * rows, rows)], act_ref.at[pl.ds(i * rows, rows)], sems.at[i]
        )
        for i in range(STEPS)
    ]
    bring_weight = weight_copies(weight_hbm, weight_ref, weight_sems, 0)
    bring_table.start()
    for copy in bring + bring_weight:
        copy.start()
    bring_table.wait()
    for i, copy in enumerate(bring):
        copy.wait()
        at = slice(i * rows, (i + 1) * rows)
        low = jnp.dot(act_ref[at, :HALF], table_ref[...], preferred_element_type=jnp.float32)
        high = jnp.dot(act_ref[at, HALF:], table_ref[...], preferred_element_type=jnp.float32)
        out_ref[at, :HALF] = (low + high).astype(jnp.bfloat16)
        out_ref[at, HALF:] = (low - high).astype(jnp.bfloat16)
    for copy in bring_weight:
        copy.wait()


def rotate(activations, weight):
    table = jnp.asarray(np.kron(sylvester(32), paley_matrix()), jnp.bfloat16)
    hbm = pl.BlockSpec(memory_space=pltpu.HBM)
    vmem = pl.BlockSpec(memory_space=pltpu.VMEM)
    half = jax.ShapeDtypeStruct((weight.shape[0], LATER), weight.dtype)
    return pl.pallas_call(
        rotate_kernel,
        in_specs=[hbm] * 3,
        out_specs=[vmem] * 2,
        out_shape=[jax.ShapeDtypeStruct(activations.shape, jnp.bfloat16), half],
        scratch_shapes=[
            pltpu.VMEM(activations.shape, jnp.bfloat16),
            pltpu.VMEM(table.shape, jnp.bfloat16),
            pltpu.SemaphoreType.DMA((STEPS + 1,)),
            pltpu.SemaphoreType.DMA((PIECES,)),
        ],
        name="rotate",
        compiler_params=small(8),
    )(*[pltpu.with_memory_space_constraint(value, pltpu.HBM) for value in (activations, table, weight)])


def sine_coefs():
    nodes = np.cos(np.pi * (np.arange(400) + 0.5) / 400) * 0.125 + 0.125
    x = np.sqrt(nodes)
    values = np.sin(2 * np.pi * x) / (2 * np.pi * x)
    return np.polynomial.chebyshev.Chebyshev.fit(
        nodes, values, 7, domain=[0, 0.25]
    ).convert(kind=np.polynomial.Polynomial).coef


COEFS = [float(c) for c in sine_coefs()]


def snap(levels):
    rest = levels - jnp.round(levels)
    square = rest * rest
    poly = jnp.full_like(square, COEFS[-1])
    for coef in COEFS[-2::-1]:
        poly = poly * square + coef
    return levels - rest * poly


def quantize_kernel(mixed_ref, weight_hbm, out_ref, weight_ref, rot_ref, weight_sems, *, norm):
    bring_weight = weight_copies(weight_hbm, weight_ref, weight_sems, LATER)
    for copy in bring_weight:
        copy.start()
    groups, rows, width = mixed_ref.shape
    lanes = 128
    sub = 16
    for row in range(0, rows, sub):
        def mix(c, top, row=row):
            at = pl.ds(pl.multiple_of(c * lanes, lanes), lanes)
            v = [mixed_ref[e, row : row + sub, at].astype(jnp.float32) for e in range(groups)]
            stride = 1
            while stride < groups:
                for e in range(groups):
                    if not e & stride:
                        v[e], v[e + stride] = v[e] + v[e + stride], v[e] - v[e + stride]
                stride *= 2
            for e in range(groups):
                rot_ref[e, row : row + sub, at] = v[e]
                top = jnp.maximum(top, jnp.abs(v[e]))
            return top

        top = lax.fori_loop(0, width // lanes, mix, jnp.zeros((sub, lanes), jnp.float32))
        scale = jnp.maximum(jnp.max(top, axis=1, keepdims=True) * norm, 1.0)
        into = jnp.broadcast_to((7.0 * norm) / scale, (sub, lanes))
        back = jnp.broadcast_to(scale / 7.0, (sub, lanes))

        def quant(c, carry, row=row, into=into, back=back):
            at = pl.ds(pl.multiple_of(c * lanes, lanes), lanes)
            for e in range(groups):
                levels = rot_ref[e, row : row + sub, at] * into
                out_ref[groups - 1 - e, row : row + sub, at] = (snap(levels) * back).astype(jnp.bfloat16)
            return carry

        lax.fori_loop(0, width // lanes, quant, 0)
    for copy in bring_weight:
        copy.wait()


def quantize(mixed, weight, norm):
    vmem = pl.BlockSpec(memory_space=pltpu.VMEM)
    half = jax.ShapeDtypeStruct((weight.shape[0], weight.shape[1] - LATER), weight.dtype)
    return pl.pallas_call(
        functools.partial(quantize_kernel, norm=norm),
        in_specs=[vmem, pl.BlockSpec(memory_space=pltpu.HBM)],
        out_specs=[vmem] * 2,
        out_shape=[jax.ShapeDtypeStruct(mixed.shape, jnp.bfloat16), half],
        scratch_shapes=[pltpu.VMEM(mixed.shape, jnp.float32), pltpu.SemaphoreType.DMA((PIECES,))],
        name="quantize",
        compiler_params=small(8),
    )(mixed, pltpu.with_memory_space_constraint(weight, pltpu.HBM))


SIDE = 4


def shift(value, along, by):
    pairs = []
    for z in range(SIDE):
        for y in range(SIDE):
            to = ((z + by) % SIDE, y) if along == "z" else (z, (y + by) % SIDE)
            pairs.append((SIDE * z + y, SIDE * to[0] + to[1]))
    return lax.ppermute(value, "tensor", pairs)


def project_kernel(place_ref, values_ref, weight_ref, first_ref, second_ref, lhs_ref, *, along, send):
    z, y = place_ref[0], place_ref[1]
    rows = values_ref.shape[0] // (SIDE * SIDE)
    group = SIDE * rows
    base = 1 if send else 3
    for r in range(3):
        for other in range(SIDE):
            ahead = ((z if along == "z" else y) + base + r) % SIDE
            owner = SIDE * ahead + other if along == "z" else SIDE * other + ahead
            start = pl.multiple_of((SIDE * SIDE - 1 - owner) * rows, rows)
            to = r * group + other * rows
            lhs_ref[to : to + rows, :] = values_ref[pl.ds(start, rows), :]
    half = weight_ref.shape[1] // 2
    for start, base in ((group, 0), (0, half)):
        for at in range(base, base + half, TILE):
            to = min(at + TILE, base + half)
            both = jnp.dot(
                lhs_ref[start : start + 2 * group, :],
                weight_ref[:, at:to],
                preferred_element_type=jnp.float32,
            ).astype(jnp.bfloat16)
            first_ref[:, at:to] = both[:group]
            second_ref[:, at:to] = both[group:]


TILE = 512


def project(values, weight, place, along, send):
    count_rows, width = values.shape
    group = count_rows // SIDE
    out = jax.ShapeDtypeStruct((group, weight.shape[1]), jnp.bfloat16)
    vmem = pl.BlockSpec(memory_space=pltpu.VMEM)
    return pl.pallas_call(
        functools.partial(project_kernel, along=along, send=send),
        in_specs=[pl.BlockSpec(memory_space=pltpu.SMEM), vmem, vmem],
        out_specs=[vmem] * 2,
        out_shape=[out] * 2,
        scratch_shapes=[pltpu.VMEM((3 * group, width), jnp.bfloat16)],
        name=("send_" if send else "keep_") + along,
        compiler_params=small(8),
    )(place, values, weight)


def f32(value):
    return value.astype(jnp.float32)


def split_kernel(place_ref, first_ref, second_ref, up_ref, down_ref, up2_ref, down2_ref, *outs, index):
    at = place_ref[index]
    rows, half = outs[0].shape[0], outs[0].shape[1] // 2
    low, high = slice(0, half), slice(half, 2 * half)
    for r in range(SIDE):
        take = pl.ds(pl.multiple_of(((at + r) % SIDE) * rows, rows), rows)
        outs[r][:, low] = (
            f32(first_ref[take, low]) + f32(down_ref[take, low]) + f32(up2_ref[take, :])
        ).astype(jnp.bfloat16)
        outs[r][:, high] = (
            f32(second_ref[take, high]) + f32(up_ref[take, high]) + f32(down2_ref[take, :])
        ).astype(jnp.bfloat16)


def split(place, index, first, second, up, down, up2, down2):
    vmem = pl.BlockSpec(memory_space=pltpu.VMEM)
    out = jax.ShapeDtypeStruct((first.shape[0] // SIDE, first.shape[1]), jnp.bfloat16)
    return pl.pallas_call(
        functools.partial(split_kernel, index=index),
        in_specs=[pl.BlockSpec(memory_space=pltpu.SMEM)] + [vmem] * 6,
        out_specs=[vmem] * 4,
        out_shape=[out] * 4,
        name="split",
        compiler_params=small(),
    )(place, first, second, up, down, up2, down2)


def relay_kernel(first_ref, second_ref, up_ref, down_ref, up2_ref, down2_ref):
    half = up2_ref.shape[1]
    up2_ref[...] = (f32(second_ref[:, :half]) + f32(up_ref[:, :half])).astype(jnp.bfloat16)
    down2_ref[...] = (f32(first_ref[:, half:]) + f32(down_ref[:, half:])).astype(jnp.bfloat16)


def relay(first, second, up, down):
    vmem = pl.BlockSpec(memory_space=pltpu.VMEM)
    out = jax.ShapeDtypeStruct((first.shape[0], first.shape[1] // 2), jnp.bfloat16)
    return pl.pallas_call(
        relay_kernel, in_specs=[vmem] * 4, out_specs=[vmem] * 2, out_shape=[out] * 2, name="relay",
        compiler_params=small(),
    )(first, second, up, down)


def finish_kernel(*refs):
    out_ref = refs[-1]
    first = 0
    for at in range(2):
        some = refs[SIDE * at : SIDE * at + SIDE]
        parts = [f32(ref[...]) for ref in some]
        width = some[0].shape[1]
        out_ref[:, first : first + width] = (
            (parts[0] + parts[1]) + (parts[2] + parts[3])
        ).astype(jnp.bfloat16)
        first += width


def finish(first, second):
    vmem = pl.BlockSpec(memory_space=pltpu.VMEM)
    rows, width = first[0].shape
    out = jax.ShapeDtypeStruct((rows, width + second[0].shape[1]), jnp.bfloat16)
    return pl.pallas_call(
        finish_kernel, in_specs=[vmem] * 8, out_specs=vmem, out_shape=out, name="finish",
        compiler_params=small(),
    )(*first, *second)


def exchange(own, ahead, far, behind, along):
    return own, shift(far, along, 2), shift(ahead, along, 1), shift(behind, along, -1)


def shards(activations, down_weight):
    count_rows, shard_width = activations.shape
    groups = lax.axis_size("tensor")
    me = lax.axis_index("tensor")
    place = jnp.stack([me // SIDE, me % SIDE]).astype(jnp.int32)
    activations, place = lax.optimization_barrier((activations, place))
    blocks, weight_z = rotate(activations, down_weight)
    blocks = blocks.reshape(groups, count_rows // groups, shard_width)
    mixed = lax.all_to_all(blocks, "tensor", split_axis=0, concat_axis=0, tiled=True)
    snapped, weight_y = quantize(mixed, down_weight, 1.0 / math.sqrt(shard_width * groups))
    backwards = [list(range(groups))[::-1]]
    values = lax.all_to_all(
        snapped, "tensor", split_axis=0, concat_axis=0, tiled=True, axis_index_groups=backwards
    )
    values = values.reshape(count_rows, shard_width)
    order = (("y", weight_y), ("z", weight_z))
    sent, kept = {}, {}
    for along, weight in order:
        up, down = project(values, weight, place, along, True)
        sent[along] = shift(up, along, 1), shift(down, along, -1)
    for along, weight in order:
        kept[along] = project(values, weight, place, along, False)
    kept = lax.optimization_barrier(kept)
    ends = {}
    for along, _ in order:
        up, down = sent[along]
        up2, down2 = relay(*kept[along], up, down)
        ends[along] = (*kept[along], up, down, shift(up2, along, 1), shift(down2, along, -1))
    second_z = exchange(*split(place, 0, *ends["y"]), "z")
    second_y = exchange(*split(place, 1, *ends["z"]), "y")
    return finish(second_y, second_z)


def solution(mesh):
    placed = (P("dp", "tensor"), P("tensor", None))
    return jax.shard_map(
        shards, mesh=mesh, in_specs=placed, out_specs=P(("dp", "tensor"), None), check_vma=False
    )
```

```python
import functools
import math

import jax
import jax.numpy as jnp
import numpy as np
from jax import lax
from jax.experimental import pallas as pl
from jax.experimental.pallas import tpu as pltpu
from jax.sharding import PartitionSpec as P


def paley_matrix():
    modulus = 13
    residues = set((value * value % modulus for value in range(1, modulus)))
    jacobsthal = np.array(
        [
            [
                (
                    0.0
                    if row_at == col_at
                    else 1.0 if (col_at - row_at) % modulus in residues else -1.0
                )
                for col_at in range(modulus)
            ]
            for row_at in range(modulus)
        ]
    )
    confer = np.zeros((14, 14))
    confer[0, 1:] = 1.0
    confer[1:, 0] = 1.0
    confer[1:, 1:] = jacobsthal
    return np.kron(confer, np.array([[1.0, 1.0], [1.0, -1.0]])) + np.kron(
        np.eye(14), np.array([[1.0, -1.0], [-1.0, -1.0]])
    )


def sylvester(order):
    matrix = np.ones((1, 1))
    while matrix.shape[0] < order:
        matrix = np.kron(matrix, np.array([[1.0, 1.0], [1.0, -1.0]]))
    return matrix


def small(mebibytes=6):
    return pltpu.CompilerParams(vmem_limit_bytes=mebibytes << 20)


HALF = 896


STEPS = 4
LATER = 2816
PIECES = 4


def weight_copies(weight_ref, out_ref, sems, first):
    rows = weight_ref.shape[0] // PIECES
    return [
        pltpu.make_async_copy(
            weight_ref.at[pl.ds(i * rows, rows), pl.ds(first, out_ref.shape[1])],
            out_ref.at[pl.ds(i * rows, rows)],
            sems.at[i],
        )
        for i in range(PIECES)
    ]


def rotate_kernel(act_hbm, table_hbm, weight_hbm, out_ref, weight_ref, act_ref, table_ref, sems, weight_sems):
    rows = act_hbm.shape[0] // STEPS
    quarter = HALF // 2
    bring_table = pltpu.make_async_copy(table_hbm, table_ref.at[pl.ds(0, quarter)], sems.at[STEPS])
    bring = [
        pltpu.make_async_copy(
            act_hbm.at[pl.ds(i * rows, rows)], act_ref.at[pl.ds(i * rows, rows)], sems.at[i]
        )
        for i in range(STEPS)
    ]
    bring_weight = weight_copies(weight_hbm, weight_ref, weight_sems, 0)
    bring_table.start()
    for copy in bring + bring_weight:
        copy.start()
    bring_table.wait()
    upper = table_ref[:quarter, :]
    column = lax.broadcasted_iota(jnp.int32, (quarter, HALF), 1)
    table_ref[quarter:, :] = jnp.where(column < quarter, upper, -upper)
    for i, copy in enumerate(bring):
        copy.wait()
        at = slice(i * rows, (i + 1) * rows)
        low = jnp.dot(act_ref[at, :HALF], table_ref[...], preferred_element_type=jnp.float32)
        high = jnp.dot(act_ref[at, HALF:], table_ref[...], preferred_element_type=jnp.float32)
        out_ref[at, :HALF] = (low + high).astype(jnp.bfloat16)
        out_ref[at, HALF:] = (low - high).astype(jnp.bfloat16)
    for copy in bring_weight:
        copy.wait()


def rotate(activations, weight):
    table = jnp.asarray(np.kron(sylvester(32), paley_matrix())[: HALF // 2], jnp.bfloat16)
    hbm = pl.BlockSpec(memory_space=pltpu.HBM)
    vmem = pl.BlockSpec(memory_space=pltpu.VMEM)
    half = jax.ShapeDtypeStruct((weight.shape[0], LATER), weight.dtype)
    return pl.pallas_call(
        rotate_kernel,
        in_specs=[hbm] * 3,
        out_specs=[vmem] * 2,
        out_shape=[jax.ShapeDtypeStruct(activations.shape, jnp.bfloat16), half],
        scratch_shapes=[
            pltpu.VMEM(activations.shape, jnp.bfloat16),
            pltpu.VMEM((HALF, HALF), jnp.bfloat16),
            pltpu.SemaphoreType.DMA((STEPS + 1,)),
            pltpu.SemaphoreType.DMA((PIECES,)),
        ],
        name="rotate",
        compiler_params=small(8),
    )(*[pltpu.with_memory_space_constraint(value, pltpu.HBM) for value in (activations, table, weight)])


def sine_coefs():
    nodes = np.cos(np.pi * (np.arange(400) + 0.5) / 400) * 0.125 + 0.125
    x = np.sqrt(nodes)
    values = np.sin(2 * np.pi * x) / (2 * np.pi * x)
    return np.polynomial.chebyshev.Chebyshev.fit(
        nodes, values, 7, domain=[0, 0.25]
    ).convert(kind=np.polynomial.Polynomial).coef


COEFS = [float(c) for c in sine_coefs()]


def snap(levels):
    rest = levels - jnp.round(levels)
    square = rest * rest
    poly = jnp.full_like(square, COEFS[-1])
    for coef in COEFS[-2::-1]:
        poly = poly * square + coef
    return levels - rest * poly


def quantize_kernel(mixed_ref, weight_hbm, out_ref, weight_ref, rot_ref, weight_sems, *, norm):
    bring_weight = weight_copies(weight_hbm, weight_ref, weight_sems, LATER)
    for copy in bring_weight:
        copy.start()
    groups, rows, width = mixed_ref.shape
    lanes = 128
    sub = 16
    for row in range(0, rows, sub):
        def mix(c, top, row=row):
            at = pl.ds(pl.multiple_of(c * lanes, lanes), lanes)
            v = [mixed_ref[e, row : row + sub, at].astype(jnp.float32) for e in range(groups)]
            stride = 1
            while stride < groups:
                for e in range(groups):
                    if not e & stride:
                        v[e], v[e + stride] = v[e] + v[e + stride], v[e] - v[e + stride]
                stride *= 2
            for e in range(groups):
                rot_ref[e, row : row + sub, at] = v[e]
                top = jnp.maximum(top, jnp.abs(v[e]))
            return top

        top = lax.fori_loop(0, width // lanes, mix, jnp.zeros((sub, lanes), jnp.float32))
        scale = jnp.maximum(jnp.max(top, axis=1, keepdims=True) * norm, 1.0)
        into = jnp.broadcast_to((7.0 * norm) / scale, (sub, lanes))
        back = jnp.broadcast_to(scale / 7.0, (sub, lanes))

        def quant(c, carry, row=row, into=into, back=back):
            at = pl.ds(pl.multiple_of(c * lanes, lanes), lanes)
            for e in range(groups):
                levels = rot_ref[e, row : row + sub, at] * into
                out_ref[groups - 1 - e, row : row + sub, at] = (snap(levels) * back).astype(jnp.bfloat16)
            return carry

        lax.fori_loop(0, width // lanes, quant, 0)
    for copy in bring_weight:
        copy.wait()


def quantize(mixed, weight, norm):
    vmem = pl.BlockSpec(memory_space=pltpu.VMEM)
    half = jax.ShapeDtypeStruct((weight.shape[0], weight.shape[1] - LATER), weight.dtype)
    return pl.pallas_call(
        functools.partial(quantize_kernel, norm=norm),
        in_specs=[vmem, pl.BlockSpec(memory_space=pltpu.HBM)],
        out_specs=[vmem] * 2,
        out_shape=[jax.ShapeDtypeStruct(mixed.shape, jnp.bfloat16), half],
        scratch_shapes=[pltpu.VMEM(mixed.shape, jnp.float32), pltpu.SemaphoreType.DMA((PIECES,))],
        name="quantize",
        compiler_params=small(8),
    )(mixed, pltpu.with_memory_space_constraint(weight, pltpu.HBM))


SIDE = 4


def shift(value, along, by):
    pairs = []
    for z in range(SIDE):
        for y in range(SIDE):
            to = ((z + by) % SIDE, y) if along == "z" else (z, (y + by) % SIDE)
            pairs.append((SIDE * z + y, SIDE * to[0] + to[1]))
    return lax.ppermute(value, "tensor", pairs)


def project_kernel(place_ref, values_ref, weight_ref, first_ref, second_ref, lhs_ref, *, along, send):
    z, y = place_ref[0], place_ref[1]
    rows = values_ref.shape[0] // (SIDE * SIDE)
    group = SIDE * rows
    base = 1 if send else 3
    for r in range(3):
        for other in range(SIDE):
            ahead = ((z if along == "z" else y) + base + r) % SIDE
            owner = SIDE * ahead + other if along == "z" else SIDE * other + ahead
            start = pl.multiple_of((SIDE * SIDE - 1 - owner) * rows, rows)
            to = r * group + other * rows
            lhs_ref[to : to + rows, :] = values_ref[pl.ds(start, rows), :]
    half = weight_ref.shape[1] // 2
    for start, base in ((group, 0), (0, half)):
        for at in range(base, base + half, TILE):
            to = min(at + TILE, base + half)
            both = jnp.dot(
                lhs_ref[start : start + 2 * group, :],
                weight_ref[:, at:to],
                preferred_element_type=jnp.float32,
            ).astype(jnp.bfloat16)
            first_ref[:, at:to] = both[:group]
            second_ref[:, at:to] = both[group:]


TILE = 512


def project(values, weight, place, along, send):
    count_rows, width = values.shape
    group = count_rows // SIDE
    out = jax.ShapeDtypeStruct((group, weight.shape[1]), jnp.bfloat16)
    vmem = pl.BlockSpec(memory_space=pltpu.VMEM)
    return pl.pallas_call(
        functools.partial(project_kernel, along=along, send=send),
        in_specs=[pl.BlockSpec(memory_space=pltpu.SMEM), vmem, vmem],
        out_specs=[vmem] * 2,
        out_shape=[out] * 2,
        scratch_shapes=[pltpu.VMEM((3 * group, width), jnp.bfloat16)],
        name=("send_" if send else "keep_") + along,
        compiler_params=small(8),
    )(place, values, weight)


def f32(value):
    return value.astype(jnp.float32)


def split_kernel(place_ref, first_ref, second_ref, up_ref, down_ref, up2_ref, down2_ref, *outs, index):
    at = place_ref[index]
    rows, half = outs[0].shape[0], outs[0].shape[1] // 2
    low, high = slice(0, half), slice(half, 2 * half)
    for r in range(SIDE):
        take = pl.ds(pl.multiple_of(((at + r) % SIDE) * rows, rows), rows)
        outs[r][:, low] = (
            f32(first_ref[take, low]) + f32(down_ref[take, low]) + f32(up2_ref[take, :])
        ).astype(jnp.bfloat16)
        outs[r][:, high] = (
            f32(second_ref[take, high]) + f32(up_ref[take, high]) + f32(down2_ref[take, :])
        ).astype(jnp.bfloat16)


def split(place, index, first, second, up, down, up2, down2):
    vmem = pl.BlockSpec(memory_space=pltpu.VMEM)
    out = jax.ShapeDtypeStruct((first.shape[0] // SIDE, first.shape[1]), jnp.bfloat16)
    return pl.pallas_call(
        functools.partial(split_kernel, index=index),
        in_specs=[pl.BlockSpec(memory_space=pltpu.SMEM)] + [vmem] * 6,
        out_specs=[vmem] * 4,
        out_shape=[out] * 4,
        name="split",
        compiler_params=small(),
    )(place, first, second, up, down, up2, down2)


def relay_kernel(own_ref, got_ref, out_ref, *, first):
    columns = slice(first, first + out_ref.shape[1])
    out_ref[...] = (f32(own_ref[:, columns]) + f32(got_ref[:, columns])).astype(jnp.bfloat16)


def relay(own, got, upper):
    vmem = pl.BlockSpec(memory_space=pltpu.VMEM)
    half = own.shape[1] // 2
    return pl.pallas_call(
        functools.partial(relay_kernel, first=half if upper else 0),
        in_specs=[vmem] * 2,
        out_specs=vmem,
        out_shape=jax.ShapeDtypeStruct((own.shape[0], half), jnp.bfloat16),
        name="relay",
        compiler_params=small(),
    )(own, got)


def finish_kernel(*refs):
    out_ref = refs[-1]
    first = 0
    for at in range(2):
        some = refs[SIDE * at : SIDE * at + SIDE]
        parts = [f32(ref[...]) for ref in some]
        width = some[0].shape[1]
        out_ref[:, first : first + width] = (
            (parts[0] + parts[1]) + (parts[2] + parts[3])
        ).astype(jnp.bfloat16)
        first += width


def finish(first, second):
    vmem = pl.BlockSpec(memory_space=pltpu.VMEM)
    rows, width = first[0].shape
    out = jax.ShapeDtypeStruct((rows, width + second[0].shape[1]), jnp.bfloat16)
    return pl.pallas_call(
        finish_kernel, in_specs=[vmem] * 8, out_specs=vmem, out_shape=out, name="finish",
        compiler_params=small(),
    )(*first, *second)


def exchange(own, ahead, far, behind, along):
    return own, shift(far, along, 2), shift(ahead, along, 1), shift(behind, along, -1)


def shards(activations, down_weight):
    count_rows, shard_width = activations.shape
    groups = lax.axis_size("tensor")
    me = lax.axis_index("tensor")
    place = jnp.stack([me // SIDE, me % SIDE]).astype(jnp.int32)
    activations, place = lax.optimization_barrier((activations, place))
    blocks, weight_z = rotate(activations, down_weight)
    blocks = blocks.reshape(groups, count_rows // groups, shard_width)
    mixed = lax.all_to_all(blocks, "tensor", split_axis=0, concat_axis=0, tiled=True)
    snapped, weight_y = quantize(mixed, down_weight, 1.0 / math.sqrt(shard_width * groups))
    backwards = [list(range(groups))[::-1]]
    values = lax.all_to_all(
        snapped, "tensor", split_axis=0, concat_axis=0, tiled=True, axis_index_groups=backwards
    )
    values = values.reshape(count_rows, shard_width)
    order = (("y", weight_y), ("z", weight_z))
    sent, kept = {}, {}
    for along, weight in order:
        up, down = project(values, weight, place, along, True)
        sent[along] = shift(up, along, 1), shift(down, along, -1)
    for along, weight in order:
        kept[along] = project(values, weight, place, along, False)
    kept = lax.optimization_barrier(kept)
    ends = {}
    for along, _ in order:
        up, down = sent[along]
        lower, upper = kept[along]
        up2, down2 = relay(upper, up, False), relay(lower, down, True)
        ends[along] = (*kept[along], up, down, shift(up2, along, 1), shift(down2, along, -1))
    second_z = exchange(*split(place, 0, *ends["y"]), "z")
    second_y = exchange(*split(place, 1, *ends["z"]), "y")
    return finish(second_y, second_z)


def solution(mesh):
    placed = (P("dp", "tensor"), P("tensor", None))
    return jax.shard_map(
        shards, mesh=mesh, in_specs=placed, out_specs=P(("dp", "tensor"), None), check_vma=False
    )
```

```python
import functools
import math

import jax
import jax.numpy as jnp
import numpy as np
from jax import lax
from jax.experimental import pallas as pl
from jax.experimental.pallas import tpu as pltpu
from jax.sharding import PartitionSpec as P


def paley_matrix():
    modulus = 13
    residues = set((value * value % modulus for value in range(1, modulus)))
    jacobsthal = np.array(
        [
            [
                (
                    0.0
                    if row_at == col_at
                    else 1.0 if (col_at - row_at) % modulus in residues else -1.0
                )
                for col_at in range(modulus)
            ]
            for row_at in range(modulus)
        ]
    )
    confer = np.zeros((14, 14))
    confer[0, 1:] = 1.0
    confer[1:, 0] = 1.0
    confer[1:, 1:] = jacobsthal
    return np.kron(confer, np.array([[1.0, 1.0], [1.0, -1.0]])) + np.kron(
        np.eye(14), np.array([[1.0, -1.0], [-1.0, -1.0]])
    )


def sylvester(order):
    matrix = np.ones((1, 1))
    while matrix.shape[0] < order:
        matrix = np.kron(matrix, np.array([[1.0, 1.0], [1.0, -1.0]]))
    return matrix


def small(mebibytes=6):
    return pltpu.CompilerParams(vmem_limit_bytes=mebibytes << 20)


HALF = 896


STEPS = 4
LATER = 2816
PIECES = 4


def weight_copies(weight_ref, out_ref, sems, first):
    rows = weight_ref.shape[0] // PIECES
    return [
        pltpu.make_async_copy(
            weight_ref.at[pl.ds(i * rows, rows), pl.ds(first, out_ref.shape[1])],
            out_ref.at[pl.ds(i * rows, rows)],
            sems.at[i],
        )
        for i in range(PIECES)
    ]


def rotate_kernel(act_hbm, table_hbm, weight_hbm, out_ref, weight_ref, act_ref, table_ref, sems, weight_sems):
    rows = act_hbm.shape[0] // STEPS
    quarter = HALF // 2
    bring_table = pltpu.make_async_copy(table_hbm, table_ref.at[pl.ds(0, quarter)], sems.at[STEPS])
    bring = [
        pltpu.make_async_copy(
            act_hbm.at[pl.ds(i * rows, rows)], act_ref.at[pl.ds(i * rows, rows)], sems.at[i]
        )
        for i in range(STEPS)
    ]
    bring_weight = weight_copies(weight_hbm, weight_ref, weight_sems, 0)
    bring_table.start()
    for copy in bring + bring_weight:
        copy.start()
    bring_table.wait()
    upper = table_ref[:quarter, :]
    column = lax.broadcasted_iota(jnp.int32, (quarter, HALF), 1)
    table_ref[quarter:, :] = jnp.where(column < quarter, upper, -upper)
    for i, copy in enumerate(bring):
        copy.wait()
        at = slice(i * rows, (i + 1) * rows)
        low = jnp.dot(act_ref[at, :HALF], table_ref[...], preferred_element_type=jnp.float32)
        high = jnp.dot(act_ref[at, HALF:], table_ref[...], preferred_element_type=jnp.float32)
        out_ref[at, :HALF] = (low + high).astype(jnp.bfloat16)
        out_ref[at, HALF:] = (low - high).astype(jnp.bfloat16)
    for copy in bring_weight:
        copy.wait()


def rotate(activations, weight):
    table = jnp.asarray(np.kron(sylvester(32), paley_matrix())[: HALF // 2], jnp.bfloat16)
    hbm = pl.BlockSpec(memory_space=pltpu.HBM)
    vmem = pl.BlockSpec(memory_space=pltpu.VMEM)
    half = jax.ShapeDtypeStruct((weight.shape[0], LATER), weight.dtype)
    return pl.pallas_call(
        rotate_kernel,
        in_specs=[hbm] * 3,
        out_specs=[vmem] * 2,
        out_shape=[jax.ShapeDtypeStruct(activations.shape, jnp.bfloat16), half],
        scratch_shapes=[
            pltpu.VMEM(activations.shape, jnp.bfloat16),
            pltpu.VMEM((HALF, HALF), jnp.bfloat16),
            pltpu.SemaphoreType.DMA((STEPS + 1,)),
            pltpu.SemaphoreType.DMA((PIECES,)),
        ],
        name="rotate",
        compiler_params=small(8),
    )(*[pltpu.with_memory_space_constraint(value, pltpu.HBM) for value in (activations, table, weight)])


def sine_coefs():
    nodes = np.cos(np.pi * (np.arange(400) + 0.5) / 400) * 0.125 + 0.125
    x = np.sqrt(nodes)
    values = np.sin(2 * np.pi * x) / (2 * np.pi * x)
    return np.polynomial.chebyshev.Chebyshev.fit(
        nodes, values, 7, domain=[0, 0.25]
    ).convert(kind=np.polynomial.Polynomial).coef


COEFS = [float(c) for c in sine_coefs()]


def snap(levels):
    rest = levels - jnp.round(levels)
    square = rest * rest
    poly = jnp.full_like(square, COEFS[-1])
    for coef in COEFS[-2::-1]:
        poly = poly * square + coef
    return levels - rest * poly


def quantize_kernel(mixed_ref, weight_hbm, out_ref, weight_ref, rot_ref, weight_sems, *, norm):
    bring_weight = weight_copies(weight_hbm, weight_ref, weight_sems, LATER)
    for copy in bring_weight:
        copy.start()
    groups, rows, width = mixed_ref.shape
    lanes = 128
    sub = 16
    for row in range(0, rows, sub):
        def mix(c, top, row=row):
            at = pl.ds(pl.multiple_of(c * lanes, lanes), lanes)
            v = [mixed_ref[e, row : row + sub, at].astype(jnp.float32) for e in range(groups)]
            stride = 1
            while stride < groups:
                for e in range(groups):
                    if not e & stride:
                        v[e], v[e + stride] = v[e] + v[e + stride], v[e] - v[e + stride]
                stride *= 2
            for e in range(groups):
                rot_ref[e, row : row + sub, at] = v[e]
                top = jnp.maximum(top, jnp.abs(v[e]))
            return top

        top = lax.fori_loop(0, width // lanes, mix, jnp.zeros((sub, lanes), jnp.float32))
        scale = jnp.maximum(jnp.max(top, axis=1, keepdims=True) * norm, 1.0)
        into = jnp.broadcast_to((7.0 * norm) / scale, (sub, lanes))
        back = jnp.broadcast_to(scale / 7.0, (sub, lanes))

        def quant(c, carry, row=row, into=into, back=back):
            at = pl.ds(pl.multiple_of(c * lanes, lanes), lanes)
            for e in range(groups):
                levels = rot_ref[e, row : row + sub, at] * into
                out_ref[groups - 1 - e, row : row + sub, at] = (snap(levels) * back).astype(jnp.bfloat16)
            return carry

        lax.fori_loop(0, width // lanes, quant, 0)
    for copy in bring_weight:
        copy.wait()


def quantize(mixed, weight, norm):
    vmem = pl.BlockSpec(memory_space=pltpu.VMEM)
    half = jax.ShapeDtypeStruct((weight.shape[0], weight.shape[1] - LATER), weight.dtype)
    return pl.pallas_call(
        functools.partial(quantize_kernel, norm=norm),
        in_specs=[vmem, pl.BlockSpec(memory_space=pltpu.HBM)],
        out_specs=[vmem] * 2,
        out_shape=[jax.ShapeDtypeStruct(mixed.shape, jnp.bfloat16), half],
        scratch_shapes=[pltpu.VMEM(mixed.shape, jnp.float32), pltpu.SemaphoreType.DMA((PIECES,))],
        name="quantize",
        compiler_params=small(8),
    )(mixed, pltpu.with_memory_space_constraint(weight, pltpu.HBM))


SIDE = 4


def shift(value, along, by):
    pairs = []
    for z in range(SIDE):
        for y in range(SIDE):
            to = ((z + by) % SIDE, y) if along == "z" else (z, (y + by) % SIDE)
            pairs.append((SIDE * z + y, SIDE * to[0] + to[1]))
    return lax.ppermute(value, "tensor", pairs)


def project_kernel(place_ref, values_ref, weight_ref, first_ref, second_ref, lhs_ref, *, along, send):
    z, y = place_ref[0], place_ref[1]
    rows = values_ref.shape[0] // (SIDE * SIDE)
    group = SIDE * rows
    base = 1 if send else 3
    for r in range(3):
        for other in range(SIDE):
            ahead = ((z if along == "z" else y) + base + r) % SIDE
            owner = SIDE * ahead + other if along == "z" else SIDE * other + ahead
            start = pl.multiple_of((SIDE * SIDE - 1 - owner) * rows, rows)
            to = r * group + other * rows
            lhs_ref[to : to + rows, :] = values_ref[pl.ds(start, rows), :]
    half = weight_ref.shape[1] // 2
    for start, base in ((group, 0), (0, half)):
        for at in range(base, base + half, TILE):
            to = min(at + TILE, base + half)
            both = jnp.dot(
                lhs_ref[start : start + 2 * group, :],
                weight_ref[:, at:to],
                preferred_element_type=jnp.float32,
            ).astype(jnp.bfloat16)
            first_ref[:, at:to] = both[:group]
            second_ref[:, at:to] = both[group:]


TILE = 1024


def project(values, weight, place, along, send):
    count_rows, width = values.shape
    group = count_rows // SIDE
    out = jax.ShapeDtypeStruct((group, weight.shape[1]), jnp.bfloat16)
    vmem = pl.BlockSpec(memory_space=pltpu.VMEM)
    return pl.pallas_call(
        functools.partial(project_kernel, along=along, send=send),
        in_specs=[pl.BlockSpec(memory_space=pltpu.SMEM), vmem, vmem],
        out_specs=[vmem] * 2,
        out_shape=[out] * 2,
        scratch_shapes=[pltpu.VMEM((3 * group, width), jnp.bfloat16)],
        name=("send_" if send else "keep_") + along,
        compiler_params=small(8),
    )(place, values, weight)


def f32(value):
    return value.astype(jnp.float32)


def split_kernel(place_ref, first_ref, second_ref, up_ref, down_ref, up2_ref, down2_ref, *outs, index):
    at = place_ref[index]
    rows, half = outs[0].shape[0], outs[0].shape[1] // 2
    low, high = slice(0, half), slice(half, 2 * half)
    for r in range(SIDE):
        take = pl.ds(pl.multiple_of(((at + r) % SIDE) * rows, rows), rows)
        outs[r][:, low] = (
            f32(first_ref[take, low]) + f32(down_ref[take, low]) + f32(up2_ref[take, :])
        ).astype(jnp.bfloat16)
        outs[r][:, high] = (
            f32(second_ref[take, high]) + f32(up_ref[take, high]) + f32(down2_ref[take, :])
        ).astype(jnp.bfloat16)


def split(place, index, first, second, up, down, up2, down2):
    vmem = pl.BlockSpec(memory_space=pltpu.VMEM)
    out = jax.ShapeDtypeStruct((first.shape[0] // SIDE, first.shape[1]), jnp.bfloat16)
    return pl.pallas_call(
        functools.partial(split_kernel, index=index),
        in_specs=[pl.BlockSpec(memory_space=pltpu.SMEM)] + [vmem] * 6,
        out_specs=[vmem] * 4,
        out_shape=[out] * 4,
        name="split",
        compiler_params=small(),
    )(place, first, second, up, down, up2, down2)


def relay_kernel(own_ref, got_ref, out_ref, *, first):
    columns = slice(first, first + out_ref.shape[1])
    out_ref[...] = (f32(own_ref[:, columns]) + f32(got_ref[:, columns])).astype(jnp.bfloat16)


def relay(own, got, upper):
    vmem = pl.BlockSpec(memory_space=pltpu.VMEM)
    half = own.shape[1] // 2
    return pl.pallas_call(
        functools.partial(relay_kernel, first=half if upper else 0),
        in_specs=[vmem] * 2,
        out_specs=vmem,
        out_shape=jax.ShapeDtypeStruct((own.shape[0], half), jnp.bfloat16),
        name="relay",
        compiler_params=small(),
    )(own, got)


def finish_kernel(*refs):
    out_ref = refs[-1]
    first = 0
    for at in range(2):
        some = refs[SIDE * at : SIDE * at + SIDE]
        parts = [f32(ref[...]) for ref in some]
        width = some[0].shape[1]
        out_ref[:, first : first + width] = (
            (parts[0] + parts[1]) + (parts[2] + parts[3])
        ).astype(jnp.bfloat16)
        first += width


def finish(first, second):
    vmem = pl.BlockSpec(memory_space=pltpu.VMEM)
    rows, width = first[0].shape
    out = jax.ShapeDtypeStruct((rows, width + second[0].shape[1]), jnp.bfloat16)
    return pl.pallas_call(
        finish_kernel, in_specs=[vmem] * 8, out_specs=vmem, out_shape=out, name="finish",
        compiler_params=small(),
    )(*first, *second)


def exchange(own, ahead, far, behind, along):
    return own, shift(far, along, 2), shift(ahead, along, 1), shift(behind, along, -1)


def shards(activations, down_weight):
    count_rows, shard_width = activations.shape
    groups = lax.axis_size("tensor")
    me = lax.axis_index("tensor")
    place = jnp.stack([me // SIDE, me % SIDE]).astype(jnp.int32)
    activations, place = lax.optimization_barrier((activations, place))
    blocks, weight_z = rotate(activations, down_weight)
    blocks = blocks.reshape(groups, count_rows // groups, shard_width)
    mixed = lax.all_to_all(blocks, "tensor", split_axis=0, concat_axis=0, tiled=True)
    snapped, weight_y = quantize(mixed, down_weight, 1.0 / math.sqrt(shard_width * groups))
    backwards = [list(range(groups))[::-1]]
    values = lax.all_to_all(
        snapped, "tensor", split_axis=0, concat_axis=0, tiled=True, axis_index_groups=backwards
    )
    values = values.reshape(count_rows, shard_width)
    order = (("y", weight_y), ("z", weight_z))
    sent, kept = {}, {}
    for along, weight in order:
        up, down = project(values, weight, place, along, True)
        sent[along] = shift(up, along, 1), shift(down, along, -1)
    for along, weight in order:
        kept[along] = project(values, weight, place, along, False)
    kept = lax.optimization_barrier(kept)
    ends = {}
    for along, _ in order:
        up, down = sent[along]
        lower, upper = kept[along]
        up2, down2 = relay(upper, up, False), relay(lower, down, True)
        ends[along] = (*kept[along], up, down, shift(up2, along, 1), shift(down2, along, -1))
    second_z = exchange(*split(place, 0, *ends["y"]), "z")
    second_y = exchange(*split(place, 1, *ends["z"]), "y")
    return finish(second_y, second_z)


def solution(mesh):
    placed = (P("dp", "tensor"), P("tensor", None))
    return jax.shard_map(
        shards, mesh=mesh, in_specs=placed, out_specs=P(("dp", "tensor"), None), check_vma=False
    )
```
